32 devices in a mesh: agent: 4 (over x, core), tile: 8 (over z, y).
Axes of the slice: x: 2, y: 2, z: 4, core: 2. Of those that a mesh axis runs over, the one named last changes fastest.
Arguments:
- states: float32 [4, 4, 512, 512], P('agent', None, 'tile'), may hold values from -6 to 6
- sinogram: float32 [256, 4, 128], P('tile'), may hold values from -6 to 6
- blocks: bfloat16 [2048, 128, 128], P('tile'), may hold values from -0.1875 to 0.1875
- block_angle: int32 [2048], P('tile'), may hold values from 0 to 63
- block_detector: int32 [2048], P('tile'), may hold values from 0 to 3
- block_tile: int32 [2048], P('tile'), may hold values from 0 to 255
- conv_first: bfloat16 [3, 3, 3, 32], replicated, may hold values from -3 to 3
- conv_hidden: bfloat16 [3, 2, 3, 3, 32, 32], replicated, may hold values from -0.5 to 0.5
- conv_last: bfloat16 [3, 3, 3, 32], replicated, may hold values from -0.375 to 0.375
Outputs:
- new_states: float32 [4, 4, 512, 512], P('agent', None, 'tile')
The draws below stay inside these ranges and needn't reach their ends.
Inputs may be any that keep to these rules, and one draw needn't show every extreme that they name: `block_angle`: each block's angle index. `block_detector`: each block's detector block. `block_tile`: tile index among the 256 pixel tiles of the block's device.
All inputs are finite; a program needn't handle non-finite values.
Results may differ from the reference program's by a relative error of at most 0.0051.
Values may be sent and summed in bfloat16 or wider, within the bound.
A program may use at most 256 MiB of HBM per device.

```python
import jax
import jax.numpy as jnp
from jax import lax

IMG = 512
SLICES = 4
ANGLES = 64
NB_DEV = 256
WIDTH = 32
MID_LAYERS = 2
DATA_STEPS = 2
TILES_DEV = 256
RAY_BLOCKS = 256
BLOCKS = 2048
BLOCKS_PER_RAY = 8


def with_ends(values, own_key, least, largest):
    place = [jax.random.randint(jax.random.fold_in(own_key, axis), (), 0, length) for axis, length in enumerate(values.shape)]
    main_axis = values.shape.index(max(values.shape))
    neighbour = place[:main_axis] + [(place[main_axis] + 1) % values.shape[main_axis]] + place[main_axis + 1:]
    return values.at[tuple(place)].set(least).at[tuple(neighbour)].set(largest)


def level_of(key, extent, shards, low, top_value):
    level, own = 1.0, jax.random.fold_in(key, 6)
    for dim, parts in shards:
        heights = jnp.exp(jax.random.uniform(jax.random.fold_in(own, dim), (parts,), jnp.float32, low / len(shards), top_value / len(shards)))
        level = level * jnp.repeat(heights, extent[dim] // parts).reshape([-1 if axis == dim else 1 for axis in range(len(extent))])
    return level


def noise(key, extent, scale, most, cuts=(), kind=jnp.bfloat16):
    drawn = jax.random.normal(key, extent, jnp.float32) * scale
    if len(cuts) > 0:
        drawn = level_of(key, extent, cuts, -0.22, 0.18) * drawn
    return jnp.clip(drawn, min=-most, max=most).astype(kind)


def setup_inputs(seed: int = 0) -> dict:
    keys = jax.random.split(jax.random.key(seed), 10)
    states = noise(keys[0], (4, SLICES, IMG, IMG), 1.0, 6.0, ((0, 4), (2, 8)), jnp.float32)
    sinogram = noise(keys[1], (RAY_BLOCKS, SLICES, 128), 1.0, 6.0, ((0, 8),), jnp.float32)
    blocks = noise(keys[2], (BLOCKS, 128, 128), (128 * BLOCKS_PER_RAY) ** -0.5, 0.1875, ((0, 8),))
    block_angle = with_ends(jax.random.randint(keys[3], (BLOCKS,), 0, ANGLES), jax.random.fold_in(keys[3], 1), 0, ANGLES - 1).astype(jnp.int32)
    block_detector = with_ends(jax.random.randint(keys[4], (BLOCKS,), 0, IMG // 128), jax.random.fold_in(keys[4], 1), 0, (IMG // 128) - 1).astype(jnp.int32)
    block_tile = with_ends(jax.random.randint(keys[5], (BLOCKS,), 0, TILES_DEV), jax.random.fold_in(keys[5], 1), 0, TILES_DEV - 1).astype(jnp.int32)
    conv_first = noise(keys[6], (3, 3, 3, WIDTH), 4 ** -0.5, 3.0)
    conv_hidden = noise(keys[7], (3, MID_LAYERS, 3, 3, WIDTH, WIDTH), (9 * WIDTH // 2) ** -0.5, 0.5)
    conv_last = noise(keys[8], (3, 3, 3, WIDTH), (9 * WIDTH) ** -0.5, 0.375)
    return {"states": states, "sinogram": sinogram, "blocks": blocks, "block_angle": block_angle, "block_detector": block_detector, "block_tile": block_tile, "conv_first": conv_first, "conv_hidden": conv_hidden, "conv_last": conv_last}


def conv_plane(feature, weight):
    padded = jnp.pad(feature.astype(jnp.float32), ((0, 0), (1, 1), (1, 1)))
    row_count = feature.shape[1]
    columns = feature.shape[2]
    weight_float = weight.astype(jnp.float32)
    summed = jnp.zeros((weight.shape[3], row_count, columns), jnp.float32)
    for offset_row in range(3):
        for offset_column in range(3):
            window = padded[:, offset_row:offset_row + row_count, offset_column:offset_column + columns]
            summed = summed + jnp.einsum("cd,cab->dab", weight_float[offset_row, offset_column], window, precision=lax.Precision.HIGHEST)
    return summed


def denoise_plane(single_plane, first, hidden, last):
    feature = single_plane[None]
    feature = jnp.maximum(conv_plane(feature, first[:, :, None, :]), 0.0).astype(jnp.bfloat16)
    for layer_index in range(hidden.shape[0]):
        feature = jnp.maximum(conv_plane(feature, hidden[layer_index]), 0.0).astype(jnp.bfloat16)
    return conv_plane(feature, last[:, :, :, None])[0]


def denoise_volume(volume, orient, conv_first, conv_hidden, conv_last):
    rounded = volume.astype(jnp.bfloat16)
    if orient == 0:
        planes = rounded
    elif orient == 1:
        planes = jnp.transpose(rounded, (2, 0, 1))
    else:
        planes = jnp.transpose(rounded, (1, 0, 2))
    result = lax.map(lambda single_plane: denoise_plane(single_plane, conv_first[orient], conv_hidden[orient], conv_last[orient]), planes)
    if orient == 0:
        return result
    if orient == 1:
        return jnp.transpose(result, (1, 2, 0))
    return jnp.transpose(result, (1, 0, 2))


def reference(states, sinogram, blocks, block_angle, block_detector, block_tile, conv_first, conv_hidden, conv_last):
    tiles_per_row = IMG // 128
    ray_index = (block_angle * tiles_per_row + block_detector).astype(jnp.int32)
    owner_device = (jnp.arange(BLOCKS, dtype=jnp.int32) // NB_DEV).astype(jnp.int32)
    pixel_index = (owner_device * TILES_DEV + block_tile).astype(jnp.int32)
    blocks_float = blocks.astype(jnp.float32)
    x_data = states[0]
    for step_index in range(DATA_STEPS):
        pixels = x_data.astype(jnp.bfloat16).reshape(SLICES, IMG * IMG // 128, 128)
        picked = jnp.take(pixels, pixel_index, axis=1).astype(jnp.float32)
        projected = jnp.einsum("zbp,bqp->bzq", picked, blocks_float, precision=lax.Precision.HIGHEST)
        ray_sums = jax.ops.segment_sum(projected, ray_index, num_segments=RAY_BLOCKS)
        residual = (ray_sums - sinogram).astype(jnp.bfloat16)
        spread = jnp.take(residual, ray_index, axis=0).astype(jnp.float32)
        contribution = jnp.einsum("bzq,bqp->bzp", spread, blocks_float, precision=lax.Precision.HIGHEST)
        summed = jax.ops.segment_sum(contribution, pixel_index, num_segments=IMG * IMG // 128)
        back_projected = jnp.transpose(summed, (1, 0, 2)).reshape(SLICES, IMG, IMG)
        x_data = x_data - 0.8 * back_projected
    fixed_points = [x_data]
    for orient in range(3):
        net_volume = denoise_volume(states[orient + 1], orient, conv_first, conv_hidden, conv_last)
        fixed_points.append(states[orient + 1] - net_volume)
    reflected = []
    for agent_index in range(4):
        reflected.append(2.0 * fixed_points[agent_index] - states[agent_index])
    average = (reflected[0] + reflected[1] + reflected[2] + reflected[3]) / 4.0
    results = []
    for agent_index in range(4):
        results.append(0.5 * states[agent_index] + 0.5 * (2.0 * average - reflected[agent_index]))
    return jnp.stack(results, axis=0)
```

```python
import functools

import jax
import jax.numpy as jnp
import numpy as np
from jax import lax
from jax.experimental import pallas as pl
from jax.experimental.pallas import tpu as pltpu
from jax.sharding import PartitionSpec as P

DATA_STEPS = 2
MESH = pl.DeviceIdType.MESH
LANES = 128
GROUPS = 16
STRIPS = 16


def extended(cells, axis, dim, width):
    count = lax.axis_size(axis)
    ends = count - 1
    head = lax.slice_in_dim(cells, 0, width, axis=dim)
    tail = lax.slice_in_dim(cells, cells.shape[dim] - width, cells.shape[dim], axis=dim)
    return jnp.concatenate(
        [
            lax.ppermute(tail, axis, [(i, (i + 1) % count) for i in range(ends)]),
            cells,
            lax.ppermute(head, axis, [((i + 1) % count, i) for i in range(ends)]),
        ],
        axis=dim,
    )


def band(weight, rows_in, first_row):
    taps_row = np.zeros((3, rows_in, 4), np.float32)
    for row_in in range(rows_in):
        for row in range(4):
            tap = row_in + first_row - row + 1
            if 0 <= tap < 3:
                taps_row[tap, row_in, row] = 1
    return spread(weight, taps_row)


def band_same(weight):
    parts = []
    for tap in range(3):
        taps_row = np.zeros((3, 4, 4), np.float32)
        taps_row[tap] = np.eye(4)
        parts.append(spread(weight, taps_row))
    return jnp.stack(parts)


def spread(weight, taps_row):
    taps_position = np.zeros((3, 4, 2), np.float32)
    for k in range(4):
        for par in range(2):
            if 0 <= k - par < 3:
                taps_position[k - par, k, par] = 1
    half = jnp.einsum("irs,ijcd->jrscd", jnp.asarray(taps_row, jnp.bfloat16), weight, preferred_element_type=jnp.float32)
    full = jnp.einsum(
        "jkp,jrscd->krcpsd", jnp.asarray(taps_position, jnp.bfloat16), half.astype(jnp.bfloat16), preferred_element_type=jnp.float32
    )
    return full.astype(jnp.bfloat16)


def net_weights(first, hidden, last, axial):
    inner = hidden.shape[-1]
    depth = 16 * inner
    if axial:
        w_first = band_same(first[:, :, None, :]).reshape(48, 8 * inner)
    else:
        w_first = band(first[:, :, None, :], 4, 0).reshape(16, 8 * inner)

    def both(weight, wide):
        if axial:
            return band_same(weight).reshape(3 * depth, wide)
        return band(weight, 4, 0).reshape(depth, wide)

    w_hidden = jnp.stack([both(hidden[l], 8 * inner) for l in range(hidden.shape[0])])
    w_last = jnp.tile(both(last[:, :, :, None], 8), (1, GROUPS))
    return w_first, w_hidden, w_last


def net_kernel(plan, x_ref, w1_ref, wh_ref, wl_ref, out_ref, even, odd):
    group, size, layers, masked, first_out, out_chunks = plan
    chunks = x_ref.shape[0]
    pairs = chunks * group
    step_rows = group * size

    if masked:
        place = lax.axis_index("tile")
        at_start = place == 0
        at_end = place == lax.axis_size("tile") - 1

    for side in range(2):
        for ref in (even, odd):
            ref[side, 0] = jnp.zeros(ref.shape[2:], ref.dtype)
            ref[side, pairs + 1] = jnp.zeros(ref.shape[2:], ref.dtype)

    def store(side, c, y):
        y = jnp.maximum(y, 0.0)
        if masked:
            outside = (at_start & (c < first_out)) | (at_end & (c >= chunks - first_out))
            y = y * jnp.where(outside, 0.0, 1.0)
        y = y.astype(jnp.bfloat16)
        even[side, pl.ds(1 + c * group, group)] = y[:, :LANES].reshape(group, size, LANES)
        odd[side, pl.ds(1 + c * group, group)] = y[:, LANES:].reshape(group, size, LANES)

    def gathered(side, c):
        low = c * group
        sources = ((odd, low), (even, low + 1), (odd, low + 1), (even, low + 2))
        parts = [ref[side, pl.ds(at, group)].reshape(step_rows, LANES) for ref, at in sources]
        return jnp.concatenate(parts, axis=1)

    def first_step(c, carry):
        y = lax.dot_general(
            x_ref[c], w1_ref[...], (((0,), (0,)), ((), ())), preferred_element_type=jnp.float32
        )
        store(0, c, y)
        return carry

    lax.fori_loop(0, chunks, first_step, 0)
    for layer in range(layers):
        source, target = layer % 2, (layer + 1) % 2

        def hidden_step(c, carry):
            y = jnp.dot(gathered(source, c), wh_ref[layer], preferred_element_type=jnp.float32)
            store(target, c, y)
            return carry

        lax.fori_loop(0, chunks, hidden_step, 0)

    lane_group = lax.broadcasted_iota(jnp.int32, (step_rows, LANES), 1) // 8

    def last_step(c, carry):
        y = jnp.dot(gathered(layers % 2, c + first_out), wl_ref[...], preferred_element_type=jnp.float32)
        out_ref[c // GROUPS] = jnp.where(lane_group == c % GROUPS, y, out_ref[c // GROUPS])
        return carry

    out_ref[...] = jnp.zeros_like(out_ref)
    lax.fori_loop(0, out_chunks, last_step, 0)


def run_net(x, weights, group, size, masked, first_out, out_chunks):
    w_first, w_hidden, w_last = weights
    chunks = x.shape[0]
    pairs = chunks * group
    layers = w_hidden.shape[0]
    out_blocks = -(-out_chunks // GROUPS)
    plan = (group, size, layers, masked, first_out, out_chunks)
    whole = pl.BlockSpec(memory_space=pltpu.VMEM)
    cells = pairs * size * 2 * LANES
    return pl.pallas_call(
        functools.partial(net_kernel, plan),
        out_shape=jax.ShapeDtypeStruct((out_blocks, group * size, LANES), jnp.float32),
        in_specs=[whole] * 4,
        out_specs=whole,
        scratch_shapes=[
            pltpu.VMEM((2, pairs + 2, size, LANES), jnp.bfloat16),
            pltpu.VMEM((2, pairs + 2, size, LANES), jnp.bfloat16),
        ],
        cost_estimate=pl.CostEstimate(flops=cells * 512 * 2 * 3, bytes_accessed=x.size * 2, transcendentals=0),
        compiler_params=pltpu.CompilerParams(vmem_limit_bytes=60 * 1024 * 1024),
        name="net_masked" if masked else "net_plain",
    )(x, w_first, w_hidden, w_last)


def axial_kernel(plan, x_ref, w1_ref, wh_ref, wl_ref, out_ref, even, odd):
    group, layers, halo = plan
    rows, _, cells = x_ref.shape
    pairs = cells // STRIPS
    step_rows = group * cells
    place = lax.axis_index("tile")
    at_start = place == 0
    at_end = place == lax.axis_size("tile") - 1
    strip = lax.broadcasted_iota(jnp.int32, (STRIPS, LANES), 0)

    for side in range(2):
        for ref in (even, odd):
            ref[side, 0] = jnp.zeros(ref.shape[2:], ref.dtype)
            ref[side, rows + 1] = jnp.zeros(ref.shape[2:], ref.dtype)

    def store(side, row, count, y):
        outside = (at_start & (row < halo)) | (at_end & (row >= rows - halo))
        y = jnp.maximum(y, 0.0) * jnp.where(outside, 0.0, 1.0)
        y = y.reshape(count, pairs, STRIPS, 2 * LANES)
        at = pl.ds(row + 1, count)
        even[side, at, pl.ds(1, pairs)] = y[..., :LANES].astype(jnp.bfloat16)
        odd[side, at, pl.ds(1, pairs)] = y[..., LANES:].astype(jnp.bfloat16)
        for r in range(count):
            before = y[r, pairs - 1, :, LANES:]
            before = jnp.where(strip == 0, 0.0, pltpu.roll(before, 1, 0))
            odd[side, row + 1 + r, 0] = before.astype(jnp.bfloat16)
            after = y[r, 0, :, :LANES]
            after = jnp.where(strip == STRIPS - 1, 0.0, pltpu.roll(after, STRIPS - 1, 0))
            even[side, row + 1 + r, pairs + 1] = after.astype(jnp.bfloat16)

    def gathered(side, row):
        parts = []
        for tap in range(3):
            at = pl.ds(row + tap, group)
            for ref, first in ((odd, 0), (even, 1), (odd, 1), (even, 2)):
                parts.append(ref[side, at, pl.ds(first, pairs)].reshape(step_rows, LANES))
        return jnp.concatenate(parts, axis=1)

    def first_step(row, carry):
        y = lax.dot_general(
            x_ref[row], w1_ref[...], (((0,), (0,)), ((), ())), preferred_element_type=jnp.float32
        )
        store(0, row, 1, y)
        return carry

    lax.fori_loop(0, rows, first_step, 0)
    for layer in range(layers):
        source, target = layer % 2, (layer + 1) % 2

        def hidden_step(c, carry):
            y = jnp.dot(gathered(source, c * group), wh_ref[layer], preferred_element_type=jnp.float32)
            store(target, c * group, group, y)
            return carry

        lax.fori_loop(0, rows // group, hidden_step, 0)

    lane_group = lax.broadcasted_iota(jnp.int32, (step_rows, LANES), 1) // 8

    def last_step(c, carry):
        y = jnp.dot(gathered(layers % 2, halo + c * group), wl_ref[...], preferred_element_type=jnp.float32)
        out_ref[c // GROUPS] = jnp.where(lane_group == c % GROUPS, y, out_ref[c // GROUPS])
        return carry

    out_ref[...] = jnp.zeros_like(out_ref)
    lax.fori_loop(0, (rows - 2 * halo) // group, last_step, 0)


def axial_net(rimmed, weights, halo):
    slices, rows, columns = rimmed.shape
    group = 4
    local = rows - 2 * halo
    pairs = columns // (2 * STRIPS)
    cells = pairs * STRIPS
    column = jnp.arange(columns, dtype=jnp.int32)[:, None, None, None]
    k = jnp.arange(4, dtype=jnp.int32)[None, :, None, None]
    i = jnp.arange(pairs, dtype=jnp.int32)[None, None, :, None]
    j = jnp.arange(STRIPS, dtype=jnp.int32)[None, None, None, :]
    place = (column == j * (2 * pairs) + 2 * i + k - 1).astype(jnp.bfloat16).reshape(columns, 4, cells)
    padded = jnp.pad(rimmed, ((0, 0), (1, 1), (0, 0)))
    x = jnp.einsum("zrc,ckm->kzrm", padded, place, preferred_element_type=jnp.float32).astype(jnp.bfloat16)
    x = jnp.stack([x[:, :, tap : tap + rows] for tap in range(3)])
    x = jnp.transpose(x, (3, 0, 1, 2, 4)).reshape(rows, 12 * slices, cells)
    layers = weights[1].shape[0]
    whole = pl.BlockSpec(memory_space=pltpu.VMEM)
    out_chunks = local // group
    out = pl.pallas_call(
        functools.partial(axial_kernel, (group, layers, halo)),
        out_shape=jax.ShapeDtypeStruct((-(-out_chunks // GROUPS), group * cells, LANES), jnp.float32),
        in_specs=[whole] * 4,
        out_specs=whole,
        scratch_shapes=[
            pltpu.VMEM((2, rows + 2, pairs + 2, STRIPS, LANES), jnp.bfloat16),
            pltpu.VMEM((2, rows + 2, pairs + 2, STRIPS, LANES), jnp.bfloat16),
        ],
        compiler_params=pltpu.CompilerParams(vmem_limit_bytes=60 * 1024 * 1024),
        name="net_axial",
    )(x, *weights)
    out = out.astype(jnp.bfloat16).reshape(out.shape[0], group, cells, LANES)
    out = jnp.swapaxes(out, 2, 3).reshape(out.shape[0], group, GROUPS, 2, slices, cells)
    net = jnp.einsum("bgqpzm,cpm->zbqgc", out, place[:, 1:3], preferred_element_type=jnp.float32)
    return net.reshape(slices, -1, columns)[:, :local]


def sagittal_net(rimmed, weights, halo):
    slices, rows, columns = rimmed.shape
    padded = jnp.pad(rimmed, ((0, 0), (1, 1), (0, 0)))
    x = jnp.stack([padded[:, k : k + rows : 2] for k in range(4)], axis=0)
    x = jnp.transpose(x, (2, 0, 1, 3)).reshape(rows // 2, 4 * slices, columns)
    local = rows - 2 * halo
    out = run_net(x, weights, 1, columns, True, halo // 2, local // 2)
    out = out.reshape(out.shape[0], columns, GROUPS, 2, slices)
    return jnp.transpose(out, (4, 0, 2, 3, 1)).reshape(slices, -1, columns)[:, :local]


def coronal_net(rounded, weights):
    slices, rows, columns = rounded.shape
    group = 512 // rows
    chunks = columns // (2 * group)
    turned = jnp.transpose(jnp.pad(rounded, ((0, 0), (0, 0), (1, 1))), (2, 0, 1))
    x = jnp.stack([turned[k : k + columns : 2] for k in range(4)], axis=1)
    x = x.reshape(chunks, group, 4 * slices, rows)
    x = jnp.transpose(x, (0, 2, 1, 3)).reshape(chunks, 4 * slices, group * rows)
    out = run_net(x, weights, group, rows, False, 0, chunks)
    out = out.reshape(out.shape[0], group, rows, GROUPS, 2, slices)
    return jnp.transpose(out, (5, 2, 0, 3, 1, 4)).reshape(slices, rows, -1)[:, :, :columns]


def ray_kernel(count, part_ref, sino_ref, out_ref, got, fresh, send1, recv1, send2, recv2):
    rows = sino_ref.shape[0]
    agent = lax.axis_index("agent")

    @pl.when(agent == 0)
    def _():
        me = lax.axis_index("tile")
        barrier = pltpu.get_barrier_semaphore()
        for d in range(1, count):
            pl.semaphore_signal(barrier, inc=1, device_id=(agent, lax.rem(me + d, count)), device_id_type=MESH)
        pl.semaphore_wait(barrier, count - 1)

        def part_copy(d):
            peer = lax.rem(me + d, count)
            return pltpu.make_async_remote_copy(
                src_ref=part_ref.at[peer],
                dst_ref=got.at[d],
                send_sem=send1.at[d],
                recv_sem=recv1.at[d],
                device_id=(agent, peer),
                device_id_type=MESH,
            )

        for d in range(1, count):
            part_copy(d).start()
        total = part_ref[me].astype(jnp.float32) - sino_ref[...]
        for d in range(1, count):
            part_copy(d).wait_recv()
            total = total + got[d].astype(jnp.float32)
        fresh[...] = total.astype(jnp.bfloat16)

        def rest_copy(d):
            return pltpu.make_async_remote_copy(
                src_ref=fresh,
                dst_ref=got2_slot(me),
                send_sem=send2.at[d],
                recv_sem=recv2.at[d],
                device_id=(agent, lax.rem(me + d, count)),
                device_id_type=MESH,
            )

        def got2_slot(slot):
            return out_ref.at[slot]

        for d in range(1, count):
            rest_copy(d).start()
        out_ref[me] = fresh[...]
        for d in range(1, count):
            rest_copy(d).wait_recv()
        for d in range(1, count):
            part_copy(d).wait_send()
            rest_copy(d).wait_send()

    @pl.when(agent != 0)
    def _():
        out_ref[...] = jnp.zeros_like(out_ref)


def ray_exchange(part, sinogram, count):
    rows = sinogram.shape[0]
    whole = pl.BlockSpec(memory_space=pltpu.VMEM)
    return pl.pallas_call(
        functools.partial(ray_kernel, count),
        out_shape=jax.ShapeDtypeStruct((count, rows, LANES), jnp.bfloat16),
        in_specs=[whole] * 2,
        out_specs=whole,
        scratch_shapes=[
            pltpu.VMEM((count, rows, LANES), jnp.bfloat16),
            pltpu.VMEM((rows, LANES), jnp.bfloat16),
            pltpu.SemaphoreType.DMA((count,)),
            pltpu.SemaphoreType.DMA((count,)),
            pltpu.SemaphoreType.DMA((count,)),
            pltpu.SemaphoreType.DMA((count,)),
        ],
        compiler_params=pltpu.CompilerParams(collective_id=0, has_side_effects=True),
        name="ray_exchange",
    )(part, sinogram)


def agent_kernel(count, own_ref, out_ref, got, send, recv):
    me = lax.axis_index("agent")
    tile = lax.axis_index("tile")
    barrier = pltpu.get_barrier_semaphore()
    for d in range(1, count):
        pl.semaphore_signal(barrier, inc=1, device_id=(lax.rem(me + d, count), tile), device_id_type=MESH)
    pl.semaphore_wait(barrier, count - 1)

    def copy(d):
        return pltpu.make_async_remote_copy(
            src_ref=own_ref,
            dst_ref=got.at[d],
            send_sem=send.at[d],
            recv_sem=recv.at[d],
            device_id=(lax.rem(me + d, count), tile),
            device_id_type=MESH,
        )

    for d in range(1, count):
        copy(d).start()
    for d in range(1, count):
        copy(d).wait_recv()
    for d in range(1, count):
        copy(d).wait_send()

    out_ref[...] = jnp.zeros_like(out_ref)
    for d in range(1, count):
        out_ref[...] += got[d].astype(jnp.float32)


def agent_sum(own, count):
    whole = pl.BlockSpec(memory_space=pltpu.VMEM)
    return pl.pallas_call(
        functools.partial(agent_kernel, count),
        out_shape=jax.ShapeDtypeStruct(own.shape, jnp.float32),
        in_specs=[whole],
        out_specs=whole,
        scratch_shapes=[
            pltpu.VMEM((count,) + own.shape, jnp.bfloat16),
            pltpu.SemaphoreType.DMA((count,)),
            pltpu.SemaphoreType.DMA((count,)),
        ],
        compiler_params=pltpu.CompilerParams(collective_id=1, has_side_effects=True),
        name="agent_sum",
    )(own)


def per_device(
    states,
    sinogram,
    blocks,
    block_angle,
    block_detector,
    block_tile,
    conv_first,
    conv_hidden,
    conv_last,
):
    current = states[0]
    slices, local_rows, image_columns = current.shape
    tile_count = lax.axis_size("tile")
    agent_count = lax.axis_size("agent")
    agent_place = lax.axis_index("agent")
    is_data = agent_place == 0
    tiles_here = local_rows * image_columns // LANES
    rays_here = sinogram.shape[0]
    ray_total = rays_here * tile_count
    part_shape = (tile_count, rays_here * slices, LANES)

    def ray_hot():
        ray_index = block_angle * (image_columns // LANES) + block_detector
        return ray_index[:, None] == jnp.arange(ray_total, dtype=jnp.int32)[None, :]

    def tile_hot():
        return block_tile[:, None] == jnp.arange(tiles_here, dtype=jnp.int32)[None, :]

    def project(volume):
        pixels = volume.astype(jnp.bfloat16).reshape(slices, tiles_here, LANES)
        picked = jnp.einsum(
            "bt,ztp->bzp", tile_hot().astype(jnp.bfloat16), pixels, preferred_element_type=jnp.float32
        ).astype(jnp.bfloat16)
        projected = jnp.einsum("bzp,bqp->bzq", picked, blocks, preferred_element_type=jnp.float32)
        partial_value = jnp.einsum(
            "br,bzq->rzq",
            ray_hot().astype(jnp.float32),
            projected,
            precision=lax.Precision.HIGHEST,
        )
        return partial_value.astype(jnp.bfloat16).reshape(part_shape)

    def spread_back(residual):
        residual = residual.reshape(ray_total, slices, LANES)
        picked = jnp.einsum(
            "br,rzq->bzq", ray_hot().astype(jnp.bfloat16), residual, preferred_element_type=jnp.float32
        ).astype(jnp.bfloat16)
        contribution = jnp.einsum("bzq,bqp->bzp", picked, blocks, preferred_element_type=jnp.float32)
        summed = jnp.einsum(
            "bt,bzp->ztp",
            tile_hot().astype(jnp.float32),
            contribution,
            precision=lax.Precision.HIGHEST,
        )
        return summed.reshape(slices, local_rows, image_columns)

    halo = conv_hidden.shape[1] + 2
    rounded = current.astype(jnp.bfloat16)
    rimmed = extended(rounded, "tile", 1, halo)
    no_part = jnp.zeros(part_shape, jnp.bfloat16)

    def reflect_of(net):
        return 2.0 * (current - net) - current

    def weights_of(o):
        return net_weights(conv_first[o], conv_hidden[o], conv_last[o], o == 0)

    def data_start():
        return project(current), current

    def axial_only():
        return no_part, reflect_of(axial_net(rimmed, weights_of(0), halo))

    def sagittal_only():
        return no_part, reflect_of(sagittal_net(rimmed, weights_of(1), halo))

    def coronal_only():
        return no_part, reflect_of(coronal_net(rounded, weights_of(2)))

    part, held = lax.switch(agent_place, [data_start, axial_only, sagittal_only, coronal_only])
    own_sinogram = sinogram.reshape(rays_here * slices, LANES)

    for step in range(DATA_STEPS):
        residual = ray_exchange(part, own_sinogram, tile_count)
        if step < DATA_STEPS - 1:

            def advance(held, residual):
                moved = held - 0.8 * spread_back(residual)
                return project(moved), moved

            part, held = lax.cond(is_data, advance, lambda h, r: (no_part, h), held, residual)
        else:

            def settle(held, residual):
                moved = held - 0.8 * spread_back(residual)
                return 2.0 * moved - current

            reflect = lax.cond(is_data, settle, lambda h, r: h, held, residual)

    sent = reflect.astype(jnp.bfloat16).reshape(slices * local_rows, image_columns)
    others = agent_sum(sent, agent_count).reshape(reflect.shape)
    new_states = 0.5 * current + 0.25 * others - 0.25 * reflect
    return new_states[None]


def solution(mesh):
    placed = (
        P("agent", None, "tile", None),
        P("tile", None, None),
        P("tile", None, None),
        P("tile"),
        P("tile"),
        P("tile"),
        P(),
        P(),
        P(),
    )
    return jax.shard_map(
        per_device,
        mesh=mesh,
        in_specs=placed,
        out_specs=P("agent", None, "tile", None),
        check_vma=False,
    )
```

```python
import functools

import jax
import jax.numpy as jnp
import numpy as np
from jax import lax
from jax.experimental import pallas as pl
from jax.experimental.pallas import tpu as pltpu
from jax.sharding import PartitionSpec as P

DATA_STEPS = 2
MESH = pl.DeviceIdType.MESH
LANES = 128
GROUPS = 16
STRIPS = 16


def extended(cells, axis, dim, width):
    count = lax.axis_size(axis)
    ends = count - 1
    head = lax.slice_in_dim(cells, 0, width, axis=dim)
    tail = lax.slice_in_dim(cells, cells.shape[dim] - width, cells.shape[dim], axis=dim)
    return jnp.concatenate(
        [
            lax.ppermute(tail, axis, [(i, (i + 1) % count) for i in range(ends)]),
            cells,
            lax.ppermute(head, axis, [((i + 1) % count, i) for i in range(ends)]),
        ],
        axis=dim,
    )


def band(weight, rows_in, first_row):
    taps_row = np.zeros((3, rows_in, 4), np.float32)
    for row_in in range(rows_in):
        for row in range(4):
            tap = row_in + first_row - row + 1
            if 0 <= tap < 3:
                taps_row[tap, row_in, row] = 1
    return spread(weight, taps_row)


def band_same(weight):
    parts = []
    for tap in range(3):
        taps_row = np.zeros((3, 4, 4), np.float32)
        taps_row[tap] = np.eye(4)
        parts.append(spread(weight, taps_row))
    return jnp.stack(parts)


def spread(weight, taps_row):
    taps_position = np.zeros((3, 4, 2), np.float32)
    for k in range(4):
        for par in range(2):
            if 0 <= k - par < 3:
                taps_position[k - par, k, par] = 1
    half = jnp.einsum("irs,ijcd->jrscd", jnp.asarray(taps_row, jnp.bfloat16), weight, preferred_element_type=jnp.float32)
    full = jnp.einsum(
        "jkp,jrscd->krcpsd", jnp.asarray(taps_position, jnp.bfloat16), half.astype(jnp.bfloat16), preferred_element_type=jnp.float32
    )
    return full.astype(jnp.bfloat16)


def hidden_band(weight):
    layers, _, _, inner, _ = weight.shape
    padded = jnp.pad(jnp.swapaxes(weight, 1, 2), ((0, 0), (1, 1), (2, 2), (0, 0), (0, 0)))
    parts = [padded[:, 1 - par : 5 - par, 3 - row : 7 - row] for par in range(2) for row in range(4)]
    return jnp.concatenate(parts, axis=-1).reshape(layers, 16 * inner, 8 * inner)


def hidden_same(weight):
    layers, _, _, inner, _ = weight.shape
    padded = jnp.pad(weight, ((0, 0), (0, 0), (1, 1), (0, 0), (0, 0)))
    wide = jnp.concatenate([padded[:, :, 1 - par : 5 - par] for par in range(2) for _ in range(4)], axis=-1)
    lane_row = (np.arange(8 * inner) // inner) % 4
    mask = jnp.asarray(lane_row[None, :] == np.arange(4)[:, None])
    full = jnp.where(mask[:, None, :], wide[:, :, :, None], jnp.zeros((), wide.dtype))
    return full.reshape(layers, 48 * inner, 8 * inner)


def net_weights(first, hidden, last, axial):
    inner = hidden.shape[-1]
    depth = 16 * inner
    if axial:
        w_first = band_same(first[:, :, None, :]).reshape(48, 8 * inner)
    else:
        w_first = band(first[:, :, None, :], 4, 0).reshape(16, 8 * inner)

    def last_part(weight):
        if axial:
            return band_same(weight).reshape(3 * depth, 8)
        return band(weight, 4, 0).reshape(depth, 8)

    w_hidden = hidden_same(hidden) if axial else hidden_band(hidden)
    w_last = jnp.tile(last_part(last[:, :, :, None]), (1, GROUPS))
    return w_first, w_hidden, w_last


def net_kernel(plan, x_ref, w1_ref, wh_ref, wl_ref, out_ref, even, odd):
    group, size, layers, masked, first_out, out_chunks = plan
    chunks = x_ref.shape[0]
    pairs = chunks * group
    step_rows = group * size

    if masked:
        place = lax.axis_index("tile")
        at_start = place == 0
        at_end = place == lax.axis_size("tile") - 1

    for side in range(2):
        for ref in (even, odd):
            ref[side, 0] = jnp.zeros(ref.shape[2:], ref.dtype)
            ref[side, pairs + 1] = jnp.zeros(ref.shape[2:], ref.dtype)

    def store(side, c, y):
        y = jnp.maximum(y, 0.0)
        if masked:
            outside = (at_start & (c < first_out)) | (at_end & (c >= chunks - first_out))
            y = y * jnp.where(outside, 0.0, 1.0)
        y = y.astype(jnp.bfloat16)
        even[side, pl.ds(1 + c * group, group)] = y[:, :LANES].reshape(group, size, LANES)
        odd[side, pl.ds(1 + c * group, group)] = y[:, LANES:].reshape(group, size, LANES)

    def gathered(side, c):
        low = c * group
        sources = ((odd, low), (even, low + 1), (odd, low + 1), (even, low + 2))
        parts = [ref[side, pl.ds(at, group)].reshape(step_rows, LANES) for ref, at in sources]
        return jnp.concatenate(parts, axis=1)

    def first_step(c, carry):
        y = lax.dot_general(
            x_ref[c], w1_ref[...], (((0,), (0,)), ((), ())), preferred_element_type=jnp.float32
        )
        store(0, c, y)
        return carry

    lax.fori_loop(0, chunks, first_step, 0)
    for layer in range(layers):
        source, target = layer % 2, (layer + 1) % 2

        def hidden_step(c, carry):
            y = jnp.dot(gathered(source, c), wh_ref[layer], preferred_element_type=jnp.float32)
            store(target, c, y)
            return carry

        lax.fori_loop(0, chunks, hidden_step, 0)

    lane_group = lax.broadcasted_iota(jnp.int32, (step_rows, LANES), 1) // 8

    def last_step(c, carry):
        y = jnp.dot(gathered(layers % 2, c + first_out), wl_ref[...], preferred_element_type=jnp.float32)
        out_ref[c // GROUPS] = jnp.where(lane_group == c % GROUPS, y, out_ref[c // GROUPS])
        return carry

    out_ref[...] = jnp.zeros_like(out_ref)
    lax.fori_loop(0, out_chunks, last_step, 0)


def run_net(x, weights, group, size, masked, first_out, out_chunks):
    w_first, w_hidden, w_last = weights
    chunks = x.shape[0]
    pairs = chunks * group
    layers = w_hidden.shape[0]
    out_blocks = -(-out_chunks // GROUPS)
    plan = (group, size, layers, masked, first_out, out_chunks)
    whole = pl.BlockSpec(memory_space=pltpu.VMEM)
    cells = pairs * size * 2 * LANES
    return pl.pallas_call(
        functools.partial(net_kernel, plan),
        out_shape=jax.ShapeDtypeStruct((out_blocks, group * size, LANES), jnp.float32),
        in_specs=[whole] * 4,
        out_specs=whole,
        scratch_shapes=[
            pltpu.VMEM((2, pairs + 2, size, LANES), jnp.bfloat16),
            pltpu.VMEM((2, pairs + 2, size, LANES), jnp.bfloat16),
        ],
        cost_estimate=pl.CostEstimate(flops=cells * 512 * 2 * 3, bytes_accessed=x.size * 2, transcendentals=0),
        compiler_params=pltpu.CompilerParams(vmem_limit_bytes=60 * 1024 * 1024),
        name="net_masked" if masked else "net_plain",
    )(x, w_first, w_hidden, w_last)


def axial_kernel(plan, x_ref, w1_ref, wh_ref, wl_ref, out_ref, even, odd):
    group, layers, halo = plan
    rows, _, cells = x_ref.shape
    pairs = cells // STRIPS
    step_rows = group * cells
    place = lax.axis_index("tile")
    at_start = place == 0
    at_end = place == lax.axis_size("tile") - 1
    strip = lax.broadcasted_iota(jnp.int32, (STRIPS, LANES), 0)

    for side in range(2):
        for ref in (even, odd):
            ref[side, 0] = jnp.zeros(ref.shape[2:], ref.dtype)
            ref[side, rows + 1] = jnp.zeros(ref.shape[2:], ref.dtype)

    def store(side, row, count, y):
        outside = (at_start & (row < halo)) | (at_end & (row >= rows - halo))
        y = jnp.maximum(y, 0.0) * jnp.where(outside, 0.0, 1.0)
        y = y.reshape(count, pairs, STRIPS, 2 * LANES)
        at = pl.ds(row + 1, count)
        even[side, at, pl.ds(1, pairs)] = y[..., :LANES].astype(jnp.bfloat16)
        odd[side, at, pl.ds(1, pairs)] = y[..., LANES:].astype(jnp.bfloat16)
        for r in range(count):
            before = y[r, pairs - 1, :, LANES:]
            before = jnp.where(strip == 0, 0.0, pltpu.roll(before, 1, 0))
            odd[side, row + 1 + r, 0] = before.astype(jnp.bfloat16)
            after = y[r, 0, :, :LANES]
            after = jnp.where(strip == STRIPS - 1, 0.0, pltpu.roll(after, STRIPS - 1, 0))
            even[side, row + 1 + r, pairs + 1] = after.astype(jnp.bfloat16)

    def gathered(side, row):
        parts = []
        for tap in range(3):
            at = pl.ds(row + tap, group)
            for ref, first in ((odd, 0), (even, 1), (odd, 1), (even, 2)):
                parts.append(ref[side, at, pl.ds(first, pairs)].reshape(step_rows, LANES))
        return jnp.concatenate(parts, axis=1)

    def first_step(row, carry):
        y = lax.dot_general(
            x_ref[row], w1_ref[...], (((0,), (0,)), ((), ())), preferred_element_type=jnp.float32
        )
        store(0, row, 1, y)
        return carry

    lax.fori_loop(0, rows, first_step, 0)
    for layer in range(layers):
        source, target = layer % 2, (layer + 1) % 2

        def hidden_step(c, carry):
            y = jnp.dot(gathered(source, c * group), wh_ref[layer], preferred_element_type=jnp.float32)
            store(target, c * group, group, y)
            return carry

        lax.fori_loop(0, rows // group, hidden_step, 0)

    lane_group = lax.broadcasted_iota(jnp.int32, (step_rows, LANES), 1) // 8

    def last_step(c, carry):
        y = jnp.dot(gathered(layers % 2, halo + c * group), wl_ref[...], preferred_element_type=jnp.float32)
        out_ref[c // GROUPS] = jnp.where(lane_group == c % GROUPS, y, out_ref[c // GROUPS])
        return carry

    out_ref[...] = jnp.zeros_like(out_ref)
    lax.fori_loop(0, (rows - 2 * halo) // group, last_step, 0)


def axial_net(rimmed, weights, halo):
    slices, rows, columns = rimmed.shape
    group = 4
    local = rows - 2 * halo
    pairs = columns // (2 * STRIPS)
    cells = pairs * STRIPS
    column = jnp.arange(columns, dtype=jnp.int32)[:, None, None, None]
    k = jnp.arange(4, dtype=jnp.int32)[None, :, None, None]
    i = jnp.arange(pairs, dtype=jnp.int32)[None, None, :, None]
    j = jnp.arange(STRIPS, dtype=jnp.int32)[None, None, None, :]
    place = (column == j * (2 * pairs) + 2 * i + k - 1).astype(jnp.bfloat16).reshape(columns, 4, cells)
    padded = jnp.pad(rimmed, ((0, 0), (1, 1), (0, 0)))
    x = jnp.einsum("zrc,ckm->kzrm", padded, place, preferred_element_type=jnp.float32).astype(jnp.bfloat16)
    x = jnp.stack([x[:, :, tap : tap + rows] for tap in range(3)])
    x = jnp.transpose(x, (3, 0, 1, 2, 4)).reshape(rows, 12 * slices, cells)
    layers = weights[1].shape[0]
    whole = pl.BlockSpec(memory_space=pltpu.VMEM)
    out_chunks = local // group
    out = pl.pallas_call(
        functools.partial(axial_kernel, (group, layers, halo)),
        out_shape=jax.ShapeDtypeStruct((-(-out_chunks // GROUPS), group * cells, LANES), jnp.float32),
        in_specs=[whole] * 4,
        out_specs=whole,
        scratch_shapes=[
            pltpu.VMEM((2, rows + 2, pairs + 2, STRIPS, LANES), jnp.bfloat16),
            pltpu.VMEM((2, rows + 2, pairs + 2, STRIPS, LANES), jnp.bfloat16),
        ],
        compiler_params=pltpu.CompilerParams(vmem_limit_bytes=60 * 1024 * 1024),
        name="net_axial",
    )(x, *weights)
    out = out.astype(jnp.bfloat16).reshape(out.shape[0], group, cells, LANES)
    out = jnp.swapaxes(out, 2, 3).reshape(out.shape[0], group, GROUPS, 2, slices, cells)
    net = jnp.einsum("bgqpzm,cpm->zbqgc", out, place[:, 1:3], preferred_element_type=jnp.float32)
    return net.reshape(slices, -1, columns)[:, :local]


def sagittal_net(rimmed, weights, halo):
    slices, rows, columns = rimmed.shape
    padded = jnp.pad(rimmed, ((0, 0), (1, 1), (0, 0)))
    x = jnp.stack([padded[:, k : k + rows : 2] for k in range(4)], axis=0)
    x = jnp.transpose(x, (2, 0, 1, 3)).reshape(rows // 2, 4 * slices, columns)
    local = rows - 2 * halo
    out = run_net(x, weights, 1, columns, True, halo // 2, local // 2)
    out = out.reshape(out.shape[0], columns, GROUPS, 2, slices)
    return jnp.transpose(out, (4, 0, 2, 3, 1)).reshape(slices, -1, columns)[:, :local]


def coronal_net(rounded, weights):
    slices, rows, columns = rounded.shape
    group = 512 // rows
    chunks = columns // (2 * group)
    turned = jnp.transpose(jnp.pad(rounded, ((0, 0), (0, 0), (1, 1))), (2, 0, 1))
    x = jnp.stack([turned[k : k + columns : 2] for k in range(4)], axis=1)
    x = x.reshape(chunks, group, 4 * slices, rows)
    x = jnp.transpose(x, (0, 2, 1, 3)).reshape(chunks, 4 * slices, group * rows)
    out = run_net(x, weights, group, rows, False, 0, chunks)
    out = out.reshape(out.shape[0], group, rows, GROUPS, 2, slices)
    return jnp.transpose(out, (5, 2, 0, 3, 1, 4)).reshape(slices, rows, -1)[:, :, :columns]


def ray_kernel(count, part_ref, sino_ref, out_ref, got, fresh, send1, recv1, send2, recv2):
    rows = sino_ref.shape[0]
    agent = lax.axis_index("agent")

    @pl.when(agent == 0)
    def _():
        me = lax.axis_index("tile")
        barrier = pltpu.get_barrier_semaphore()
        for d in range(1, count):
            pl.semaphore_signal(barrier, inc=1, device_id=(agent, lax.rem(me + d, count)), device_id_type=MESH)
        pl.semaphore_wait(barrier, count - 1)

        def part_copy(d):
            peer = lax.rem(me + d, count)
            return pltpu.make_async_remote_copy(
                src_ref=part_ref.at[peer],
                dst_ref=got.at[d],
                send_sem=send1.at[d],
                recv_sem=recv1.at[d],
                device_id=(agent, peer),
                device_id_type=MESH,
            )

        for d in range(1, count):
            part_copy(d).start()
        total = part_ref[me].astype(jnp.float32) - sino_ref[...]
        for d in range(1, count):
            part_copy(d).wait_recv()
            total = total + got[d].astype(jnp.float32)
        fresh[...] = total.astype(jnp.bfloat16)

        def rest_copy(d):
            return pltpu.make_async_remote_copy(
                src_ref=fresh,
                dst_ref=got2_slot(me),
                send_sem=send2.at[d],
                recv_sem=recv2.at[d],
                device_id=(agent, lax.rem(me + d, count)),
                device_id_type=MESH,
            )

        def got2_slot(slot):
            return out_ref.at[slot]

        for d in range(1, count):
            rest_copy(d).start()
        out_ref[me] = fresh[...]
        for d in range(1, count):
            rest_copy(d).wait_recv()
        for d in range(1, count):
            part_copy(d).wait_send()
            rest_copy(d).wait_send()

    @pl.when(agent != 0)
    def _():
        out_ref[...] = jnp.zeros_like(out_ref)


def ray_exchange(part, sinogram, count):
    rows = sinogram.shape[0]
    whole = pl.BlockSpec(memory_space=pltpu.VMEM)
    return pl.pallas_call(
        functools.partial(ray_kernel, count),
        out_shape=jax.ShapeDtypeStruct((count, rows, LANES), jnp.bfloat16),
        in_specs=[whole] * 2,
        out_specs=whole,
        scratch_shapes=[
            pltpu.VMEM((count, rows, LANES), jnp.bfloat16),
            pltpu.VMEM((rows, LANES), jnp.bfloat16),
            pltpu.SemaphoreType.DMA((count,)),
            pltpu.SemaphoreType.DMA((count,)),
            pltpu.SemaphoreType.DMA((count,)),
            pltpu.SemaphoreType.DMA((count,)),
        ],
        compiler_params=pltpu.CompilerParams(collective_id=0, has_side_effects=True),
        name="ray_exchange",
    )(part, sinogram)


def agent_kernel(own_ref, out_ref, near, pair, far, send, recv):
    me = lax.axis_index("agent")
    tile = lax.axis_index("tile")
    partner = me + 1 - 2 * (me % 2)
    across = (me + 2) % 4
    barrier = pltpu.get_barrier_semaphore()
    for peer in (partner, across):
        pl.semaphore_signal(barrier, inc=1, device_id=(peer, tile), device_id_type=MESH)
    pl.semaphore_wait(barrier, 2)

    first = pltpu.make_async_remote_copy(
        src_ref=own_ref,
        dst_ref=near,
        send_sem=send.at[0],
        recv_sem=recv.at[0],
        device_id=(partner, tile),
        device_id_type=MESH,
    )
    first.start()
    first.wait()
    pair[...] = (own_ref[...].astype(jnp.float32) + near[...].astype(jnp.float32)).astype(jnp.bfloat16)
    second = pltpu.make_async_remote_copy(
        src_ref=pair,
        dst_ref=far,
        send_sem=send.at[1],
        recv_sem=recv.at[1],
        device_id=(across, tile),
        device_id_type=MESH,
    )
    second.start()
    second.wait()
    out_ref[...] = near[...].astype(jnp.float32) + far[...].astype(jnp.float32)


def agent_sum(own):
    whole = pl.BlockSpec(memory_space=pltpu.VMEM)
    return pl.pallas_call(
        agent_kernel,
        out_shape=jax.ShapeDtypeStruct(own.shape, jnp.float32),
        in_specs=[whole],
        out_specs=whole,
        scratch_shapes=[
            pltpu.VMEM(own.shape, jnp.bfloat16),
            pltpu.VMEM(own.shape, jnp.bfloat16),
            pltpu.VMEM(own.shape, jnp.bfloat16),
            pltpu.SemaphoreType.DMA((2,)),
            pltpu.SemaphoreType.DMA((2,)),
        ],
        compiler_params=pltpu.CompilerParams(collective_id=1, has_side_effects=True),
        name="agent_sum",
    )(own)


def per_device(
    states,
    sinogram,
    blocks,
    block_angle,
    block_detector,
    block_tile,
    conv_first,
    conv_hidden,
    conv_last,
):
    current = states[0]
    slices, local_rows, image_columns = current.shape
    tile_count = lax.axis_size("tile")
    agent_place = lax.axis_index("agent")
    is_data = agent_place == 0
    tiles_here = local_rows * image_columns // LANES
    rays_here = sinogram.shape[0]
    ray_total = rays_here * tile_count
    part_shape = (tile_count, rays_here * slices, LANES)

    def ray_hot():
        ray_index = block_angle * (image_columns // LANES) + block_detector
        return ray_index[:, None] == jnp.arange(ray_total, dtype=jnp.int32)[None, :]

    def tile_hot():
        return block_tile[:, None] == jnp.arange(tiles_here, dtype=jnp.int32)[None, :]

    def project(volume):
        pixels = volume.astype(jnp.bfloat16).reshape(slices, tiles_here, LANES)
        picked = jnp.einsum(
            "bt,ztp->bzp", tile_hot().astype(jnp.bfloat16), pixels, preferred_element_type=jnp.float32
        ).astype(jnp.bfloat16)
        projected = jnp.einsum("bzp,bqp->bzq", picked, blocks, preferred_element_type=jnp.float32)
        partial_value = jnp.einsum(
            "br,bzq->rzq",
            ray_hot().astype(jnp.float32),
            projected,
            precision=lax.Precision.HIGHEST,
        )
        return partial_value.astype(jnp.bfloat16).reshape(part_shape)

    def spread_back(residual):
        residual = residual.reshape(ray_total, slices, LANES)
        picked = jnp.einsum(
            "br,rzq->bzq", ray_hot().astype(jnp.bfloat16), residual, preferred_element_type=jnp.float32
        ).astype(jnp.bfloat16)
        contribution = jnp.einsum("bzq,bqp->bzp", picked, blocks, preferred_element_type=jnp.float32)
        summed = jnp.einsum(
            "bt,bzp->ztp",
            tile_hot().astype(jnp.float32),
            contribution,
            precision=lax.Precision.HIGHEST,
        )
        return summed.reshape(slices, local_rows, image_columns)

    halo = conv_hidden.shape[1] + 2
    rounded = current.astype(jnp.bfloat16)
    rimmed = extended(rounded, "tile", 1, halo)
    no_part = jnp.zeros(part_shape, jnp.bfloat16)

    def reflect_of(net):
        return 2.0 * (current - net) - current

    def weights_of(o):
        return net_weights(conv_first[o], conv_hidden[o], conv_last[o], o == 0)

    def data_start():
        return project(current), current

    def axial_only():
        return no_part, reflect_of(axial_net(rimmed, weights_of(0), halo))

    def sagittal_only():
        return no_part, reflect_of(sagittal_net(rimmed, weights_of(1), halo))

    def coronal_only():
        return no_part, reflect_of(coronal_net(rounded, weights_of(2)))

    part, held = lax.switch(agent_place, [data_start, axial_only, sagittal_only, coronal_only])
    own_sinogram = sinogram.reshape(rays_here * slices, LANES)

    for step in range(DATA_STEPS):
        residual = ray_exchange(part, own_sinogram, tile_count)
        if step < DATA_STEPS - 1:

            def advance(held, residual):
                moved = held - 0.8 * spread_back(residual)
                return project(moved), moved

            part, held = lax.cond(is_data, advance, lambda h, r: (no_part, h), held, residual)
        else:

            def settle(held, residual):
                moved = held - 0.8 * spread_back(residual)
                return 2.0 * moved - current

            reflect = lax.cond(is_data, settle, lambda h, r: h, held, residual)

    sent = reflect.astype(jnp.bfloat16).reshape(slices * local_rows, image_columns)
    others = agent_sum(sent).reshape(reflect.shape)
    new_states = 0.5 * current + 0.25 * others - 0.25 * reflect
    return new_states[None]


def solution(mesh):
    placed = (
        P("agent", None, "tile", None),
        P("tile", None, None),
        P("tile", None, None),
        P("tile"),
        P("tile"),
        P("tile"),
        P(),
        P(),
        P(),
    )
    return jax.shard_map(
        per_device,
        mesh=mesh,
        in_specs=placed,
        out_specs=P("agent", None, "tile", None),
        check_vma=False,
    )
```

```python
import functools

import jax
import jax.numpy as jnp
import numpy as np
from jax import lax
from jax.experimental import pallas as pl
from jax.experimental.pallas import tpu as pltpu
from jax.sharding import PartitionSpec as P

DATA_STEPS = 2
MESH = pl.DeviceIdType.MESH
LANES = 128
GROUPS = 16
STRIPS = 16


def extended(cells, axis, dim, width):
    count = lax.axis_size(axis)
    ends = count - 1
    head = lax.slice_in_dim(cells, 0, width, axis=dim)
    tail = lax.slice_in_dim(cells, cells.shape[dim] - width, cells.shape[dim], axis=dim)
    return jnp.concatenate(
        [
            lax.ppermute(tail, axis, [(i, (i + 1) % count) for i in range(ends)]),
            cells,
            lax.ppermute(head, axis, [((i + 1) % count, i) for i in range(ends)]),
        ],
        axis=dim,
    )


def band(weight, rows_in, first_row):
    taps_row = np.zeros((3, rows_in, 4), np.float32)
    for row_in in range(rows_in):
        for row in range(4):
            tap = row_in + first_row - row + 1
            if 0 <= tap < 3:
                taps_row[tap, row_in, row] = 1
    return spread(weight, taps_row)


def band_same(weight):
    parts = []
    for tap in range(3):
        taps_row = np.zeros((3, 4, 4), np.float32)
        taps_row[tap] = np.eye(4)
        parts.append(spread(weight, taps_row))
    return jnp.stack(parts)


def spread(weight, taps_row):
    taps_position = np.zeros((3, 4, 2), np.float32)
    for k in range(4):
        for par in range(2):
            if 0 <= k - par < 3:
                taps_position[k - par, k, par] = 1
    half = jnp.einsum("irs,ijcd->jrscd", jnp.asarray(taps_row, jnp.bfloat16), weight, preferred_element_type=jnp.float32)
    full = jnp.einsum(
        "jkp,jrscd->krcpsd", jnp.asarray(taps_position, jnp.bfloat16), half.astype(jnp.bfloat16), preferred_element_type=jnp.float32
    )
    return full.astype(jnp.bfloat16)


def hidden_band(weight):
    layers, _, _, inner, _ = weight.shape
    padded = jnp.pad(jnp.swapaxes(weight, 1, 2), ((0, 0), (1, 1), (2, 2), (0, 0), (0, 0)))
    parts = [padded[:, 1 - par : 5 - par, 3 - row : 7 - row] for par in range(2) for row in range(4)]
    return jnp.concatenate(parts, axis=-1).reshape(layers, 16 * inner, 8 * inner)


def hidden_same(weight):
    layers, _, _, inner, _ = weight.shape
    padded = jnp.pad(weight, ((0, 0), (0, 0), (1, 1), (0, 0), (0, 0)))
    wide = jnp.concatenate([padded[:, :, 1 - par : 5 - par] for par in range(2) for _ in range(4)], axis=-1)
    lane_row = (np.arange(8 * inner) // inner) % 4
    mask = jnp.asarray(lane_row[None, :] == np.arange(4)[:, None])
    full = jnp.where(mask[:, None, :], wide[:, :, :, None], jnp.zeros((), wide.dtype))
    return full.reshape(layers, 48 * inner, 8 * inner)


def net_weights(first, hidden, last, axial):
    inner = hidden.shape[-1]
    depth = 16 * inner
    if axial:
        w_first = band_same(first[:, :, None, :]).reshape(48, 8 * inner)
    else:
        w_first = band(first[:, :, None, :], 4, 0).reshape(16, 8 * inner)

    def last_part(weight):
        if axial:
            return band_same(weight).reshape(3 * depth, 8)
        return band(weight, 4, 0).reshape(depth, 8)

    w_hidden = hidden_same(hidden) if axial else hidden_band(hidden)
    w_last = jnp.tile(last_part(last[:, :, :, None]), (1, GROUPS))
    return w_first, w_hidden, w_last


def net_kernel(plan, x_ref, w1_ref, wh_ref, wl_ref, out_ref, even, odd):
    group, size, layers, masked, first_out, out_chunks = plan
    chunks = x_ref.shape[0]
    pairs = chunks * group
    step_rows = group * size

    if masked:
        place = lax.axis_index("tile")
        at_start = place == 0
        at_end = place == lax.axis_size("tile") - 1

    for side in range(2):
        for ref in (even, odd):
            ref[side, 0] = jnp.zeros(ref.shape[2:], ref.dtype)
            ref[side, pairs + 1] = jnp.zeros(ref.shape[2:], ref.dtype)

    def store(side, c, y):
        y = jnp.maximum(y, 0.0)
        if masked:
            outside = (at_start & (c < first_out)) | (at_end & (c >= chunks - first_out))
            y = y * jnp.where(outside, 0.0, 1.0)
        y = y.astype(jnp.bfloat16)
        even[side, pl.ds(1 + c * group, group)] = y[:, :LANES].reshape(group, size, LANES)
        odd[side, pl.ds(1 + c * group, group)] = y[:, LANES:].reshape(group, size, LANES)

    def gathered(side, c):
        low = c * group
        sources = ((odd, low), (even, low + 1), (odd, low + 1), (even, low + 2))
        parts = [ref[side, pl.ds(at, group)].reshape(step_rows, LANES) for ref, at in sources]
        return jnp.concatenate(parts, axis=1)

    def first_step(c, carry):
        y = lax.dot_general(
            x_ref[c], w1_ref[...], (((0,), (0,)), ((), ())), preferred_element_type=jnp.float32
        )
        store(0, c, y)
        return carry

    lax.fori_loop(0, chunks, first_step, 0)
    for layer in range(layers):
        source, target = layer % 2, (layer + 1) % 2

        def hidden_step(c, carry):
            y = jnp.dot(gathered(source, c), wh_ref[layer], preferred_element_type=jnp.float32)
            store(target, c, y)
            return carry

        lax.fori_loop(0, chunks, hidden_step, 0)

    lane_group = lax.broadcasted_iota(jnp.int32, (step_rows, LANES), 1) // 8

    def last_step(c, carry):
        y = jnp.dot(gathered(layers % 2, c + first_out), wl_ref[...], preferred_element_type=jnp.float32)
        out_ref[c // GROUPS] = jnp.where(lane_group == c % GROUPS, y, out_ref[c // GROUPS])
        return carry

    out_ref[...] = jnp.zeros_like(out_ref)
    lax.fori_loop(0, out_chunks, last_step, 0)


def run_net(x, weights, group, size, masked, first_out, out_chunks):
    w_first, w_hidden, w_last = weights
    chunks = x.shape[0]
    pairs = chunks * group
    layers = w_hidden.shape[0]
    out_blocks = -(-out_chunks // GROUPS)
    plan = (group, size, layers, masked, first_out, out_chunks)
    whole = pl.BlockSpec(memory_space=pltpu.VMEM)
    cells = pairs * size * 2 * LANES
    return pl.pallas_call(
        functools.partial(net_kernel, plan),
        out_shape=jax.ShapeDtypeStruct((out_blocks, group * size, LANES), jnp.float32),
        in_specs=[whole] * 4,
        out_specs=whole,
        scratch_shapes=[
            pltpu.VMEM((2, pairs + 2, size, LANES), jnp.bfloat16),
            pltpu.VMEM((2, pairs + 2, size, LANES), jnp.bfloat16),
        ],
        cost_estimate=pl.CostEstimate(flops=cells * 512 * 2 * 3, bytes_accessed=x.size * 2, transcendentals=0),
        compiler_params=pltpu.CompilerParams(vmem_limit_bytes=60 * 1024 * 1024),
        name="net_masked" if masked else "net_plain",
    )(x, w_first, w_hidden, w_last)


def axial_kernel(plan, x_ref, w1_ref, wh_ref, wl_ref, out_ref, even, odd):
    group, layers, halo = plan
    rows, _, cells = x_ref.shape
    pairs = cells // STRIPS
    step_rows = group * cells
    place = lax.axis_index("tile")
    at_start = place == 0
    at_end = place == lax.axis_size("tile") - 1
    strip = lax.broadcasted_iota(jnp.int32, (STRIPS, LANES), 0)

    for side in range(2):
        for ref in (even, odd):
            ref[side, 0] = jnp.zeros(ref.shape[2:], ref.dtype)
            ref[side, rows + 1] = jnp.zeros(ref.shape[2:], ref.dtype)

    def store(side, row, count, y):
        outside = (at_start & (row < halo)) | (at_end & (row >= rows - halo))
        y = jnp.maximum(y, 0.0) * jnp.where(outside, 0.0, 1.0)
        y = y.reshape(count, pairs, STRIPS, 2 * LANES)
        at = pl.ds(row + 1, count)
        even[side, at, pl.ds(1, pairs)] = y[..., :LANES].astype(jnp.bfloat16)
        odd[side, at, pl.ds(1, pairs)] = y[..., LANES:].astype(jnp.bfloat16)
        for r in range(count):
            before = y[r, pairs - 1, :, LANES:]
            before = jnp.where(strip == 0, 0.0, pltpu.roll(before, 1, 0))
            odd[side, row + 1 + r, 0] = before.astype(jnp.bfloat16)
            after = y[r, 0, :, :LANES]
            after = jnp.where(strip == STRIPS - 1, 0.0, pltpu.roll(after, STRIPS - 1, 0))
            even[side, row + 1 + r, pairs + 1] = after.astype(jnp.bfloat16)

    def gathered(side, row):
        parts = []
        for tap in range(3):
            at = pl.ds(row + tap, group)
            for ref, first in ((odd, 0), (even, 1), (odd, 1), (even, 2)):
                parts.append(ref[side, at, pl.ds(first, pairs)].reshape(step_rows, LANES))
        return jnp.concatenate(parts, axis=1)

    def first_step(row, carry):
        y = lax.dot_general(
            x_ref[row], w1_ref[...], (((0,), (0,)), ((), ())), preferred_element_type=jnp.float32
        )
        store(0, row, 1, y)
        return carry

    lax.fori_loop(0, rows, first_step, 0, unroll=4)
    for layer in range(layers):
        source, target = layer % 2, (layer + 1) % 2

        def hidden_step(c, carry):
            y = jnp.dot(gathered(source, c * group), wh_ref[layer], preferred_element_type=jnp.float32)
            store(target, c * group, group, y)
            return carry

        lax.fori_loop(0, rows // group, hidden_step, 0)

    lane_group = lax.broadcasted_iota(jnp.int32, (step_rows, LANES), 1) // 8

    def last_step(c, carry):
        y = jnp.dot(gathered(layers % 2, halo + c * group), wl_ref[...], preferred_element_type=jnp.float32)
        out_ref[c // GROUPS] = jnp.where(lane_group == c % GROUPS, y, out_ref[c // GROUPS])
        return carry

    out_ref[...] = jnp.zeros_like(out_ref)
    lax.fori_loop(0, (rows - 2 * halo) // group, last_step, 0)


def axial_net(rimmed, weights, halo):
    slices, rows, columns = rimmed.shape
    group = 4
    local = rows - 2 * halo
    pairs = columns // (2 * STRIPS)
    cells = pairs * STRIPS
    column = jnp.arange(columns, dtype=jnp.int32)[:, None, None, None]
    k = jnp.arange(4, dtype=jnp.int32)[None, :, None, None]
    i = jnp.arange(pairs, dtype=jnp.int32)[None, None, :, None]
    j = jnp.arange(STRIPS, dtype=jnp.int32)[None, None, None, :]
    place = (column == j * (2 * pairs) + 2 * i + k - 1).astype(jnp.bfloat16).reshape(columns, 4, cells)
    padded = jnp.pad(rimmed, ((0, 0), (1, 1), (0, 0)))
    x = jnp.einsum("zrc,ckm->kzrm", padded, place, preferred_element_type=jnp.float32).astype(jnp.bfloat16)
    x = jnp.stack([x[:, :, tap : tap + rows] for tap in range(3)])
    x = jnp.transpose(x, (3, 0, 1, 2, 4)).reshape(rows, 12 * slices, cells)
    layers = weights[1].shape[0]
    whole = pl.BlockSpec(memory_space=pltpu.VMEM)
    out_chunks = local // group
    out = pl.pallas_call(
        functools.partial(axial_kernel, (group, layers, halo)),
        out_shape=jax.ShapeDtypeStruct((-(-out_chunks // GROUPS), group * cells, LANES), jnp.float32),
        in_specs=[whole] * 4,
        out_specs=whole,
        scratch_shapes=[
            pltpu.VMEM((2, rows + 2, pairs + 2, STRIPS, LANES), jnp.bfloat16),
            pltpu.VMEM((2, rows + 2, pairs + 2, STRIPS, LANES), jnp.bfloat16),
        ],
        compiler_params=pltpu.CompilerParams(vmem_limit_bytes=60 * 1024 * 1024),
        name="net_axial",
    )(x, *weights)
    out = out.astype(jnp.bfloat16).reshape(out.shape[0], group, cells, LANES)
    out = jnp.swapaxes(out, 2, 3).reshape(out.shape[0], group, GROUPS, 2, slices, cells)
    net = jnp.einsum("bgqpzm,cpm->zbqgc", out, place[:, 1:3], preferred_element_type=jnp.float32)
    return net.reshape(slices, -1, columns)[:, :local]


def sagittal_net(rimmed, weights, halo):
    slices, rows, columns = rimmed.shape
    padded = jnp.pad(rimmed, ((0, 0), (1, 1), (0, 0)))
    x = jnp.stack([padded[:, k : k + rows : 2] for k in range(4)], axis=0)
    x = jnp.transpose(x, (2, 0, 1, 3)).reshape(rows // 2, 4 * slices, columns)
    local = rows - 2 * halo
    out = run_net(x, weights, 1, columns, True, halo // 2, local // 2)
    out = out.reshape(out.shape[0], columns, GROUPS, 2, slices)
    return jnp.transpose(out, (4, 0, 2, 3, 1)).reshape(slices, -1, columns)[:, :local]


def coronal_net(rounded, weights):
    slices, rows, columns = rounded.shape
    group = 512 // rows
    chunks = columns // (2 * group)
    turned = jnp.transpose(jnp.pad(rounded, ((0, 0), (0, 0), (1, 1))), (2, 0, 1))
    x = jnp.stack([turned[k : k + columns : 2] for k in range(4)], axis=1)
    x = x.reshape(chunks, group, 4 * slices, rows)
    x = jnp.transpose(x, (0, 2, 1, 3)).reshape(chunks, 4 * slices, group * rows)
    out = run_net(x, weights, group, rows, False, 0, chunks)
    out = out.reshape(out.shape[0], group, rows, GROUPS, 2, slices)
    return jnp.transpose(out, (5, 2, 0, 3, 1, 4)).reshape(slices, rows, -1)[:, :, :columns]


def ray_kernel(count, part_ref, sino_ref, out_ref, got, fresh, send1, recv1, send2, recv2):
    rows = sino_ref.shape[0]
    agent = lax.axis_index("agent")

    @pl.when(agent == 0)
    def _():
        me = lax.axis_index("tile")
        barrier = pltpu.get_barrier_semaphore()
        for d in range(1, count):
            pl.semaphore_signal(barrier, inc=1, device_id=(agent, lax.rem(me + d, count)), device_id_type=MESH)
        pl.semaphore_wait(barrier, count - 1)

        def part_copy(d):
            peer = lax.rem(me + d, count)
            return pltpu.make_async_remote_copy(
                src_ref=part_ref.at[peer],
                dst_ref=got.at[d],
                send_sem=send1.at[d],
                recv_sem=recv1.at[d],
                device_id=(agent, peer),
                device_id_type=MESH,
            )

        for d in range(1, count):
            part_copy(d).start()
        total = part_ref[me].astype(jnp.float32) - sino_ref[...]
        for d in range(1, count):
            part_copy(d).wait_recv()
            total = total + got[d].astype(jnp.float32)
        fresh[...] = total.astype(jnp.bfloat16)

        def rest_copy(d):
            return pltpu.make_async_remote_copy(
                src_ref=fresh,
                dst_ref=got2_slot(me),
                send_sem=send2.at[d],
                recv_sem=recv2.at[d],
                device_id=(agent, lax.rem(me + d, count)),
                device_id_type=MESH,
            )

        def got2_slot(slot):
            return out_ref.at[slot]

        for d in range(1, count):
            rest_copy(d).start()
        out_ref[me] = fresh[...]
        for d in range(1, count):
            rest_copy(d).wait_recv()
        for d in range(1, count):
            part_copy(d).wait_send()
            rest_copy(d).wait_send()

    @pl.when(agent != 0)
    def _():
        out_ref[...] = jnp.zeros_like(out_ref)


def ray_exchange(part, sinogram, count):
    rows = sinogram.shape[0]
    whole = pl.BlockSpec(memory_space=pltpu.VMEM)
    return pl.pallas_call(
        functools.partial(ray_kernel, count),
        out_shape=jax.ShapeDtypeStruct((count, rows, LANES), jnp.bfloat16),
        in_specs=[whole] * 2,
        out_specs=whole,
        scratch_shapes=[
            pltpu.VMEM((count, rows, LANES), jnp.bfloat16),
            pltpu.VMEM((rows, LANES), jnp.bfloat16),
            pltpu.SemaphoreType.DMA((count,)),
            pltpu.SemaphoreType.DMA((count,)),
            pltpu.SemaphoreType.DMA((count,)),
            pltpu.SemaphoreType.DMA((count,)),
        ],
        compiler_params=pltpu.CompilerParams(collective_id=0, has_side_effects=True),
        name="ray_exchange",
    )(part, sinogram)


def agent_kernel(own_ref, out_ref, near, pair, far, send, recv):
    me = lax.axis_index("agent")
    tile = lax.axis_index("tile")
    partner = me + 1 - 2 * (me % 2)
    across = (me + 2) % 4
    barrier = pltpu.get_barrier_semaphore()
    for peer in (partner, across):
        pl.semaphore_signal(barrier, inc=1, device_id=(peer, tile), device_id_type=MESH)
    pl.semaphore_wait(barrier, 2)

    first = pltpu.make_async_remote_copy(
        src_ref=own_ref,
        dst_ref=near,
        send_sem=send.at[0],
        recv_sem=recv.at[0],
        device_id=(partner, tile),
        device_id_type=MESH,
    )
    first.start()
    first.wait()
    pair[...] = (own_ref[...].astype(jnp.float32) + near[...].astype(jnp.float32)).astype(jnp.bfloat16)
    second = pltpu.make_async_remote_copy(
        src_ref=pair,
        dst_ref=far,
        send_sem=send.at[1],
        recv_sem=recv.at[1],
        device_id=(across, tile),
        device_id_type=MESH,
    )
    second.start()
    second.wait()
    out_ref[...] = near[...].astype(jnp.float32) + far[...].astype(jnp.float32)


def agent_sum(own):
    whole = pl.BlockSpec(memory_space=pltpu.VMEM)
    return pl.pallas_call(
        agent_kernel,
        out_shape=jax.ShapeDtypeStruct(own.shape, jnp.float32),
        in_specs=[whole],
        out_specs=whole,
        scratch_shapes=[
            pltpu.VMEM(own.shape, jnp.bfloat16),
            pltpu.VMEM(own.shape, jnp.bfloat16),
            pltpu.VMEM(own.shape, jnp.bfloat16),
            pltpu.SemaphoreType.DMA((2,)),
            pltpu.SemaphoreType.DMA((2,)),
        ],
        compiler_params=pltpu.CompilerParams(collective_id=1, has_side_effects=True),
        name="agent_sum",
    )(own)


def per_device(
    states,
    sinogram,
    blocks,
    block_angle,
    block_detector,
    block_tile,
    conv_first,
    conv_hidden,
    conv_last,
):
    current = states[0]
    slices, local_rows, image_columns = current.shape
    tile_count = lax.axis_size("tile")
    agent_place = lax.axis_index("agent")
    is_data = agent_place == 0
    tiles_here = local_rows * image_columns // LANES
    rays_here = sinogram.shape[0]
    ray_total = rays_here * tile_count
    part_shape = (tile_count, rays_here * slices, LANES)

    def ray_hot():
        ray_index = block_angle * (image_columns // LANES) + block_detector
        return ray_index[:, None] == jnp.arange(ray_total, dtype=jnp.int32)[None, :]

    def tile_hot():
        return block_tile[:, None] == jnp.arange(tiles_here, dtype=jnp.int32)[None, :]

    def project(volume):
        pixels = volume.astype(jnp.bfloat16).reshape(slices, tiles_here, LANES)
        picked = jnp.einsum(
            "bt,ztp->bzp", tile_hot().astype(jnp.bfloat16), pixels, preferred_element_type=jnp.float32
        ).astype(jnp.bfloat16)
        projected = jnp.einsum("bzp,bqp->bzq", picked, blocks, preferred_element_type=jnp.float32)
        partial_value = jnp.einsum(
            "br,bzq->rzq",
            ray_hot().astype(jnp.float32),
            projected,
            precision=lax.Precision.HIGHEST,
        )
        return partial_value.astype(jnp.bfloat16).reshape(part_shape)

    def spread_back(residual):
        residual = residual.reshape(ray_total, slices, LANES)
        picked = jnp.einsum(
            "br,rzq->bzq", ray_hot().astype(jnp.bfloat16), residual, preferred_element_type=jnp.float32
        ).astype(jnp.bfloat16)
        contribution = jnp.einsum("bzq,bqp->bzp", picked, blocks, preferred_element_type=jnp.float32)
        summed = jnp.einsum(
            "bt,bzp->ztp",
            tile_hot().astype(jnp.float32),
            contribution,
            precision=lax.Precision.HIGHEST,
        )
        return summed.reshape(slices, local_rows, image_columns)

    halo = conv_hidden.shape[1] + 2
    rounded = current.astype(jnp.bfloat16)
    rimmed = extended(rounded, "tile", 1, halo)
    no_part = jnp.zeros(part_shape, jnp.bfloat16)

    def reflect_of(net):
        return 2.0 * (current - net) - current

    def weights_of(o):
        return net_weights(conv_first[o], conv_hidden[o], conv_last[o], o == 0)

    def data_start():
        return project(current), current

    def axial_only():
        return no_part, reflect_of(axial_net(rimmed, weights_of(0), halo))

    def sagittal_only():
        return no_part, reflect_of(sagittal_net(rimmed, weights_of(1), halo))

    def coronal_only():
        return no_part, reflect_of(coronal_net(rounded, weights_of(2)))

    part, held = lax.switch(agent_place, [data_start, axial_only, sagittal_only, coronal_only])
    own_sinogram = sinogram.reshape(rays_here * slices, LANES)

    for step in range(DATA_STEPS):
        residual = ray_exchange(part, own_sinogram, tile_count)
        if step < DATA_STEPS - 1:

            def advance(held, residual):
                moved = held - 0.8 * spread_back(residual)
                return project(moved), moved

            part, held = lax.cond(is_data, advance, lambda h, r: (no_part, h), held, residual)
        else:

            def settle(held, residual):
                moved = held - 0.8 * spread_back(residual)
                return 2.0 * moved - current

            reflect = lax.cond(is_data, settle, lambda h, r: h, held, residual)

    sent = reflect.astype(jnp.bfloat16).reshape(slices * local_rows, image_columns)
    others = agent_sum(sent).reshape(reflect.shape)
    new_states = 0.5 * current + 0.25 * others - 0.25 * reflect
    return new_states[None]


def solution(mesh):
    placed = (
        P("agent", None, "tile", None),
        P("tile", None, None),
        P("tile", None, None),
        P("tile"),
        P("tile"),
        P("tile"),
        P(),
        P(),
        P(),
    )
    return jax.shard_map(
        per_device,
        mesh=mesh,
        in_specs=placed,
        out_specs=P("agent", None, "tile", None),
        check_vma=False,
    )
```
